32 devices in a mesh: rep: 1, dp: 32 (over x, y, z, core).
Axes of the slice: x: 2, y: 2, z: 4, core: 2. Of those that a mesh axis runs over, the one named last changes fastest.
Arguments:
- a: bfloat16 [32, 2, 8192, 640], P(('rep', 'dp'))
- g: bfloat16 [32, 2, 8192, 4096], P(('rep', 'dp'))
Outputs:
- output: bfloat16 [2, 640, 4096], P('rep')
All inputs are finite; a program needn't handle non-finite values.
Results may differ from the reference program's by a relative error of at most 0.012.
Values are sent between devices in bfloat16 or wider.
A program may use at most 2 GiB of HBM per device.

```python
import jax
import jax.numpy as jnp
from jax import lax

DEVICES = 32
MATRICES = 2
TOKENS = 8192
D = 640
FF = 4096


def setup_inputs(seed: int = 0, part: int = 0) -> dict:
    ka, kg, ks = (jax.random.fold_in(k, part) for k in jax.random.split(jax.random.key(seed), 3))
    size = 2.0 ** jax.random.uniform(ks, (DEVICES, MATRICES, 1, 1), jnp.float32, -1.0, 1.0)
    a = jax.random.normal(ka, (DEVICES, MATRICES, TOKENS, D), jnp.float32)
    g = size * jax.random.normal(kg, (DEVICES, MATRICES, TOKENS, FF), jnp.float32) * (DEVICES * TOKENS) ** -0.5
    return {"a": a.astype(jnp.bfloat16), "g": g.astype(jnp.bfloat16)}


def reference(a, g):
    def take(so_far, one):
        return so_far + jnp.einsum("ntd,ntf->ndf", *one, preferred_element_type=jnp.float32), None

    return lax.scan(take, jnp.zeros((MATRICES, D, FF), jnp.float32), (a, g))[0].astype(jnp.bfloat16)
```

```python
import jax
import jax.numpy as jnp
from jax import lax
from jax.experimental import pallas as pl
from jax.experimental.pallas import tpu as pltpu
from jax.sharding import PartitionSpec as P

T, D, FF, MATS = 8192, 640, 4096, 2
FC = 1024
TK = 2048
KS = T // TK
PER = FF // FC
NC = MATS * PER
NG = 3
PR = D // 16
GROUPS = (("xyw", 384), ("yxw", 384), ("wxy", 128), ("wyx", 128))
OFFSETS = (4, 5, 8, 10, 12, 15, 17, 19, 22, 23)
RS_LO = (0, 8, 12, 14, 15)
RS_N = (8, 4, 2, 1, 1)
F32, BF16 = jnp.float32, jnp.bfloat16


def kernel(a_ref, g_ref, o_ref, ab, gb, acc, *rest):
    ng = len(GROUPS)
    part, send, recv, done = (rest[i * ng:(i + 1) * ng] for i in range(4))
    asem, gsem, rs_s, rs_r, ag_s, ag_r, osem = rest[4 * ng:]
    me = lax.axis_index("dp")
    bits = {"x": me // 16, "y": (me // 8) % 2, "h": (me // 4) % 2, "w": (me // 2) % 2, "c": me % 2}
    size = {"x": 16, "y": 8, "h": 4, "w": 2, "c": 1}
    peer = {d: me + size[d] * (1 - 2 * bits[d]) for d in bits}

    def a_copy(n, k):
        rows = pl.ds(k * TK, TK)
        return pltpu.make_async_copy(a_ref.at[0, n, rows, :], ab.at[k], asem.at[k])

    def g_copy(t):
        c, k = t // KS, t % KS
        rows = pl.ds(pl.multiple_of(k * TK, TK), TK)
        cols = pl.ds(pl.multiple_of((c % PER) * FC, FC), FC)
        return pltpu.make_async_copy(g_ref.at[0, c // PER, rows, cols], gb.at[t % NG], gsem.at[t % NG])

    for k in range(KS):
        a_copy(0, k).start()
        if k < NG - 1:
            g_copy(jnp.int32(k)).start()

    barrier = pltpu.get_barrier_semaphore()
    for d in peer:
        pl.semaphore_signal(barrier, inc=1, device_id=(0, peer[d]), device_id_type=pl.DeviceIdType.MESH)
    pl.semaphore_wait(barrier, len(peer))

    def b(gi, j):
        return bits[GROUPS[gi][0][j]]

    def rs_copy(gi, ph, c):
        d = "c" if ph == 0 else "h" if ph == 4 else GROUPS[gi][0][ph - 1]
        par, where = c % 2, pl.ds(RS_LO[ph], RS_N[ph])
        return pltpu.make_async_remote_copy(
            src_ref=send[gi].at[par, where], dst_ref=recv[gi].at[par, where],
            send_sem=rs_s.at[gi, ph, par], recv_sem=rs_r.at[gi, ph, par],
            device_id=(0, peer[d]), device_id_type=pl.DeviceIdType.MESH)

    def ag_copy(gi, ph, c):
        d = "c" if ph == 3 else GROUPS[gi][0][2 - ph]
        n = 1 << ph
        first = bits["c"] * 8 if ph < 4 else 0
        for j in range(3 - ph):
            first = first + b(gi, j) * (4 >> j)
        where = pl.ds(first, n)
        return pltpu.make_async_remote_copy(
            src_ref=done[gi].at[c, where], dst_ref=done[gi].at[c, where],
            send_sem=ag_s.at[gi, ph, c], recv_sem=ag_r.at[gi, ph, c],
            device_id=(0, peer[d]), device_id_type=pl.DeviceIdType.MESH)

    def out_copy(gi, c):
        off = sum(w for _, w in GROUPS[:gi])
        cols = pl.ds(pl.multiple_of((c % PER) * FC + off, 128), GROUPS[gi][1])
        return pltpu.make_async_copy(done[gi].at[c], o_ref.at[c // PER, :, :, cols], osem.at[gi, c])

    def rows_of(piece):
        return pl.ds(pl.multiple_of(piece * PR, 8), PR)

    def stage(s, c):
        par = c % 2
        for gi, (_, w) in enumerate(GROUPS):
            off = sum(v for _, v in GROUPS[:gi])
            cols = slice(off, off + w)
            if s == 0:
                other = (1 - bits["c"]) * 8
                for j in range(8):
                    send[gi][par, j] = acc[par, rows_of(other + j), cols].astype(BF16)
                rs_copy(gi, 0, c).start()
            elif s == 1:
                rs_copy(gi, 0, c).wait()
                own = bits["c"] * 8
                keep, give = b(gi, 0) * 4, (1 - b(gi, 0)) * 4
                for j in range(4):
                    send[gi][par, 8 + j] = (acc[par, rows_of(own + give + j), cols]
                                            + recv[gi][par, give + j].astype(F32)).astype(BF16)
                rs_copy(gi, 1, c).start()
                for j in range(4):
                    part[gi][par, j] = (acc[par, rows_of(own + keep + j), cols]
                                        + recv[gi][par, keep + j].astype(F32))
            elif s in (2, 3):
                rs_copy(gi, s - 1, c).wait()
                n = 2 if s == 2 else 1
                base = 0 if s == 2 else b(gi, 1) * 2
                keep, give = b(gi, s - 1) * n, (1 - b(gi, s - 1)) * n
                lo = RS_LO[s - 1]
                for j in range(n):
                    send[gi][par, RS_LO[s] + j] = (part[gi][par, base + give + j]
                                                   + recv[gi][par, lo + give + j].astype(F32)).astype(BF16)
                rs_copy(gi, s, c).start()
                for j in range(n):
                    part[gi][par, base + keep + j] = (part[gi][par, base + keep + j]
                                                      + recv[gi][par, lo + keep + j].astype(F32))
            elif s == 4:
                rs_copy(gi, 3, c).wait()
                mine = b(gi, 1) * 2 + b(gi, 2)
                send[gi][par, 15] = (part[gi][par, mine] + recv[gi][par, 14].astype(F32)).astype(BF16)
                rs_copy(gi, 4, c).start()
            elif s == 5:
                rs_copy(gi, 4, c).wait()
                mine = bits["c"] * 8 + b(gi, 0) * 4 + b(gi, 1) * 2 + b(gi, 2)
                done[gi][c, mine] = (send[gi][par, 15].astype(F32) + recv[gi][par, 15].astype(F32)).astype(BF16)
                ag_copy(gi, 0, c).start()
            elif s in (6, 7, 8):
                ag_copy(gi, s - 6, c).wait()
                ag_copy(gi, s - 5, c).start()
            else:
                ag_copy(gi, 3, c).wait()
                out_copy(gi, c).start()

    def dot(k, slot):
        return lax.dot_general(ab[k], gb[slot], (((0,), (0,)), ((), ())), preferred_element_type=F32)

    def chunk(i, _):
        for k in range(KS):
            for s in reversed(range(len(OFFSETS))):
                if OFFSETS[s] % KS != k:
                    continue
                c = i - OFFSETS[s] // KS

                @pl.when((c >= 0) & (c < NC))
                def _():
                    stage(s, c)

            @pl.when(i < NC)
            def _():
                t = i * KS + k

                @pl.when(t + NG - 1 < NC * KS)
                def _():
                    g_copy(t + NG - 1).start()

                @pl.when(i % PER == 0)
                def _():
                    a_copy(0, k).wait()

                g_copy(t).wait()
                if k == 0:
                    acc[i % 2] = dot(k, t % NG)
                else:
                    acc[i % 2] += dot(k, t % NG)

                @pl.when(i == PER - 1)
                def _():
                    a_copy(1, k).start()
        return 0

    lax.fori_loop(0, NC + OFFSETS[-1] // KS + 0, chunk, 0)
    for gi in range(ng):
        for c in range(NC):
            out_copy(gi, c).wait()


def solution(mesh):
    ng = len(GROUPS)
    dma = pltpu.SemaphoreType.DMA
    scratch = [pltpu.VMEM((KS, TK, D), BF16), pltpu.VMEM((NG, TK, FC), BF16), pltpu.VMEM((2, D, FC), F32)]
    scratch += [pltpu.VMEM((2, 4, PR, w), F32) for _, w in GROUPS]
    scratch += [pltpu.VMEM((2, 16, PR, w), BF16) for _, w in GROUPS]
    scratch += [pltpu.VMEM((2, 16, PR, w), BF16) for _, w in GROUPS]
    scratch += [pltpu.VMEM((NC, 16, PR, w), BF16) for _, w in GROUPS]
    scratch += [dma((KS,)), dma((NG,)), dma((ng, 5, 2)), dma((ng, 5, 2)),
                dma((ng, 4, NC)), dma((ng, 4, NC)), dma((ng, NC))]

    def local(a, g):
        out = pl.pallas_call(
            kernel,
            out_shape=jax.ShapeDtypeStruct((MATS, 16, PR, FF), BF16),
            in_specs=[pl.BlockSpec(memory_space=pl.ANY)] * 2,
            out_specs=pl.BlockSpec(memory_space=pl.ANY),
            scratch_shapes=scratch,
            compiler_params=pltpu.CompilerParams(
                collective_id=0, has_side_effects=True, vmem_limit_bytes=63 * 2**20),
            name="summed_grads",
        )(a, g)
        return out.reshape(MATS, D, FF)

    spec = P(("rep", "dp"))
    return jax.shard_map(local, mesh=mesh, in_specs=(spec, spec), out_specs=P("rep"), check_vma=False)
```

```python
import jax
import jax.numpy as jnp
from jax import lax
from jax.experimental import pallas as pl
from jax.experimental.pallas import tpu as pltpu
from jax.sharding import PartitionSpec as P

T, D, FF, MATS = 8192, 640, 4096, 2
FC = 512
TK = 4096
KS = T // TK
PAIRS = MATS * FF // FC // 2
HALF = PAIRS // MATS
LOOP = PAIRS - 1
NG = 3
NA = 4
PR = D // 16
F32, BF16 = jnp.float32, jnp.bfloat16


class Plan:
    def __init__(self, groups, width, count, slots):
        self.groups, self.width, self.count, self.slots = groups, width, count, slots
        self.q = len(groups)
        self.n = [16]
        for g in groups:
            self.n.append(self.n[-1] >> len(g))
        self.lo, self.sem, at, sem = [], [], 0, 0
        for j, g in enumerate(groups):
            self.lo.append(at)
            self.sem.append(sem)
            at += ((1 << len(g)) - 1) * self.n[j + 1]
            sem += (1 << len(g)) - 1
        self.last, self.sems = at, sem
        self.stages = 2 * self.q + 2


PLANS = (
    Plan((("c",), ("x",), ("y", "w")), 512, LOOP, 2),
    Plan((("c",), ("y",), ("x", "w")), 512, LOOP, 2),
    Plan((("c",), ("x",), ("y", "w")), 512, 1, 1),
    Plan((("c",), ("y",), ("x", "w")), 256, 1, 1),
    Plan((("c",), ("x", "y", "w")), 256, 1, 1),
)
OFFSETS = ((0, 1, 3, 7, 9, 11, 13, 14), (0, 2, 4, 6, 9, 12, 14, 15))
DOT = None
ENDING = (
    (1, 0, 6), (1, 2, 5), (0, 3, 5), (1, 4, 4), (1, 5, 3), (0, 7, 3), DOT, (1, 1, 6), (0, 2, 6), (0, 5, 4), DOT,
    (2, 0, 0), (1, 3, 5), (0, 4, 5), (1, 5, 4), (2, 1, 0), (1, 6, 3), DOT, (3, 0, 0), (3, 1, 0), (1, 2, 6),
    (0, 3, 6), (1, 4, 5), (0, 6, 4), (1, 7, 3), DOT, (4, 0, 0), (2, 2, 0), (4, 1, 0), (1, 3, 6), (0, 4, 6),
    (0, 5, 5), (1, 6, 4), (0, 7, 4), (1, 7, 4), (3, 2, 0), (1, 5, 5), (2, 3, 0), (4, 2, 0), (1, 4, 6), (0, 6, 5),
    (0, 7, 5), (0, 5, 6), (3, 3, 0), (2, 4, 0), (4, 3, 0), (1, 6, 5), (1, 7, 5), (3, 4, 0), (1, 5, 6), (0, 6, 6),
    (2, 5, 0), (0, 7, 6), (4, 4, 0), (3, 5, 0), (4, 5, 0), (1, 6, 6), (2, 6, 0), (3, 6, 0), (1, 7, 6), (2, 7, 0),
    (3, 7, 0),
)
NP = len(PLANS)


def kernel(a_ref, g_ref, *rest):
    done, (ab, gb, acc), rest = rest[:NP], rest[NP:NP + 3], rest[NP + 3:]
    part, send, recv, rs_s, rs_r, ag_s, ag_r = (rest[i * NP:(i + 1) * NP] for i in range(7))
    asem, gsem = rest[7 * NP:]
    me = lax.axis_index("dp")
    bits = {"x": me // 16, "y": (me // 8) % 2, "h": (me // 4) % 2, "w": (me // 2) % 2, "c": me % 2}
    size = {"x": 16, "y": 8, "h": 4, "w": 2, "c": 1}

    def a_copy(n, k):
        rows = pl.ds(k * TK, TK)
        return pltpu.make_async_copy(a_ref.at[0, n, rows, :], ab.at[rows, :], asem.at[k])

    def g_copy(t):
        c, k = t // KS, t % KS
        rows = pl.ds(pl.multiple_of(k * TK, TK), TK)
        cols = pl.ds(pl.multiple_of((c % (2 * HALF)) * FC, FC), FC)
        return pltpu.make_async_copy(g_ref.at[0, c // (2 * HALF), rows, cols], gb.at[t % NG], gsem.at[t % NG])

    for k in range(KS):
        a_copy(0, k).start()
        g_copy(jnp.int32(k)).start()

    def flip(dims, m):
        value = 0
        for i, d in enumerate(dims):
            one = (m >> (len(dims) - 1 - i)) & 1
            value = value * 2 + (1 - bits[d] if one else bits[d])
        return value

    def peer(dims, m):
        to = me
        for i, d in enumerate(dims):
            if (m >> (len(dims) - 1 - i)) & 1:
                to = to + size[d] * (1 - 2 * bits[d])
        return (0, to)

    barrier = pltpu.get_barrier_semaphore()
    cube = ("x", "y", "w")
    partners = [peer(("c",), 1), peer(("h",), 1)] + [peer(cube, m) for m in range(1, 8)]
    for to in partners:
        pl.semaphore_signal(barrier, inc=1, device_id=to, device_id_type=pl.DeviceIdType.MESH)
    pl.semaphore_wait(barrier, len(partners))

    def remote(src, dst, ssem, rsem, to):
        return pltpu.make_async_remote_copy(
            src_ref=src, dst_ref=dst, send_sem=ssem, recv_sem=rsem,
            device_id=to, device_id_type=pl.DeviceIdType.MESH)

    def masks(plan, j):
        return range(1, 1 << len(plan.groups[j]))

    def rs_copy(pi, j, m, slot):
        plan = PLANS[pi]
        if j == plan.q:
            where, sem, to = pl.ds(plan.last, 1), plan.sems, peer(("h",), 1)
        else:
            n = plan.n[j + 1]
            where, sem, to = pl.ds(plan.lo[j] + (m - 1) * n, n), plan.sem[j] + m - 1, peer(plan.groups[j], m)
        return remote(send[pi].at[slot, where], recv[pi].at[slot, where],
                      rs_s[pi].at[sem, slot], rs_r[pi].at[sem, slot], to)

    def ag_copy(pi, j, m, c):
        plan = PLANS[pi]
        first = 0
        for i in range(j + 1):
            first = first + flip(plan.groups[i], 0) * plan.n[i + 1]
        where, sem = pl.ds(first, plan.n[j + 1]), plan.sem[j] + m - 1
        return remote(done[pi].at[c, where], done[pi].at[c, where],
                      ag_s[pi].at[sem, c], ag_r[pi].at[sem, c], peer(plan.groups[j], m))

    def stage(pi, s, c, tot):
        plan = PLANS[pi]
        q, w, slot = plan.q, plan.width, c % plan.slots

        def total(piece):
            return acc[tot, pl.ds(pl.multiple_of(piece * PR, 8), PR), :w]

        def value(p):
            v = total(flip(plan.groups[0], 0) * plan.n[1] + p) if s == 1 else part[pi][slot, p]
            for m in masks(plan, s - 1):
                v = v + recv[pi][slot, plan.lo[s - 1] + (m - 1) * plan.n[s] + p].astype(F32)
            return v

        if 1 <= s <= q:
            for m in masks(plan, s - 1):
                rs_copy(pi, s - 1, m, slot).wait()
        if s < q:
            n = plan.n[s + 1]
            for m in masks(plan, s):
                give = flip(plan.groups[s], m) * n
                for j in range(n):
                    v = total(give + j) if s == 0 else value(give + j)
                    send[pi][slot, plan.lo[s] + (m - 1) * n + j] = v.astype(BF16)
                rs_copy(pi, s, m, slot).start()
            if s > 0:
                keep = flip(plan.groups[s], 0) * n
                for j in range(n):
                    part[pi][slot, j] = value(keep + j)
        elif s == q:
            send[pi][slot, plan.last] = value(0).astype(BF16)
            rs_copy(pi, q, 0, slot).start()
        elif s == q + 1:
            rs_copy(pi, q, 0, slot).wait()
            mine = 0
            for i in range(q):
                mine = mine + flip(plan.groups[i], 0) * plan.n[i + 1]
            both = send[pi][slot, plan.last].astype(F32) + recv[pi][slot, plan.last].astype(F32)
            done[pi][c, mine] = both.astype(BF16)
        else:
            j = 2 * q + 1 - s
            for m in masks(plan, j):
                ag_copy(pi, j, m, c).wait()

    def gather(pi, s, c):
        plan = PLANS[pi]
        j = 2 * plan.q - s
        if 0 <= j < plan.q:
            for m in masks(plan, j):
                ag_copy(pi, j, m, c).start()

    def run(pi, s, c, tot):
        stage(pi, s, c, tot)
        if s > PLANS[pi].q:
            gather(pi, s, c)

    def dot(k, slot, cols):
        rows = slice(k * TK, (k + 1) * TK)
        return lax.dot_general(ab[rows, :], gb[slot, :, cols], (((0,), (0,)), ((), ())), preferred_element_type=F32)

    every = slice(0, FC)

    def pair(i, _):
        for u in range(2 * KS):
            which, k = u // KS, u % KS
            stages = [(OFFSETS[pi][s], pi, s) for pi in range(2) for s in range(PLANS[pi].stages)]
            for off, pi, s in sorted(stages, key=lambda v: (-v[0], v[1])):
                e = (pi + 1) * KS + off
                if e % (2 * KS) != u:
                    continue
                c = i - e // (2 * KS)

                @pl.when(c >= 0)
                def _():
                    run(pi, s, c, (2 * c + pi) % NA)

            t = i * 2 * KS + u
            g_copy(t + NG - 1).start()
            if which == 0:
                @pl.when(i % HALF == 0)
                def _():
                    a_copy(0, k).wait()

            g_copy(t).wait()
            tot = (2 * i + which) % NA
            if k == 0:
                acc[tot] = dot(k, t % NG, every)
            else:
                acc[tot] += dot(k, t % NG, every)
            if which == 1:
                @pl.when(i == HALF - 1)
                def _():
                    a_copy(1, k).start()
        return 0

    lax.fori_loop(0, LOOP, pair, 0)

    base = 2 * LOOP
    t0 = base * KS

    def tail_dot(step):
        if step < KS:
            if t0 + step + NG - 1 < 2 * PAIRS * KS:
                g_copy(jnp.int32(t0 + step + NG - 1)).start()
            g_copy(jnp.int32(t0 + step)).wait()
            d = dot(step, (t0 + step) % NG, every)
            if step == 0:
                acc[base % NA] = d
            else:
                acc[base % NA] += d
        else:
            part_of = step - KS
            cols = slice(part_of * 256, part_of * 256 + 256)
            for k in range(KS):
                if part_of == 0:
                    if t0 + KS + k + NG - 1 < 2 * PAIRS * KS:
                        g_copy(jnp.int32(t0 + KS + k + NG - 1)).start()
                    g_copy(jnp.int32(t0 + KS + k)).wait()
            tot = (base + 1 + part_of) % NA
            acc[tot, :, :256] = dot(0, (t0 + KS) % NG, cols) + dot(1, (t0 + KS + 1) % NG, cols)

    step = 0
    for item in ENDING:
        if item is DOT:
            tail_dot(step)
            step += 1
        else:
            pi, s, c = item
            run(pi, s, c, (2 * c + pi if pi < 2 else base + pi - 2) % NA)


def write_out(*refs):
    done, o_ref, sem = refs[:NP], refs[NP], refs[NP + 1]
    copies = []

    def copy(pi, c, at):
        w, per = PLANS[pi].width, FF
        cols = pl.ds(at % per, w)
        copies.append(pltpu.make_async_copy(
            done[pi].at[c], o_ref.at[at // per, :, :, cols], sem.at[len(copies)]))

    for c in range(LOOP):
        for pi in range(2):
            copy(pi, c, (2 * c + pi) * FC)
    at = 2 * LOOP * FC
    for pi in range(2, NP):
        copy(pi, 0, at)
        at += PLANS[pi].width
    for one in copies:
        one.start()
    for one in copies:
        one.wait()


def solution(mesh):
    dma = pltpu.SemaphoreType.DMA
    scratch = [pltpu.VMEM((T, D), BF16), pltpu.VMEM((NG, TK, FC), BF16), pltpu.VMEM((NA, D, FC), F32)]
    scratch += [pltpu.VMEM((p.slots, max(p.n[2], 1), PR, p.width), F32) for p in PLANS]
    scratch += [pltpu.VMEM((p.slots, 16, PR, p.width), BF16) for p in PLANS] * 2
    scratch += [dma((p.sems + 1, p.slots)) for p in PLANS] * 2
    scratch += [dma((p.sems, p.count)) for p in PLANS] * 2
    scratch += [dma((KS,)), dma((NG,))]
    shapes = [(p.count, 16, PR, p.width) for p in PLANS]

    def local(a, g):
        done = pl.pallas_call(
            kernel,
            out_shape=[pltpu.VMEM(s, BF16) for s in shapes],
            in_specs=[pl.BlockSpec(memory_space=pl.ANY)] * 2,
            out_specs=[pl.BlockSpec(memory_space=pltpu.VMEM)] * NP,
            scratch_shapes=scratch,
            compiler_params=pltpu.CompilerParams(
                collective_id=0, has_side_effects=True, vmem_limit_bytes=50 * 2**20),
            name="summed_grads",
        )(a, g)
        done = [pltpu.with_memory_space_constraint(d, pltpu.VMEM) for d in done]
        out = pl.pallas_call(
            write_out,
            out_shape=jax.ShapeDtypeStruct((MATS, 16, PR, FF), BF16),
            in_specs=[pl.BlockSpec(memory_space=pltpu.VMEM)] * NP,
            out_specs=pl.BlockSpec(memory_space=pl.ANY),
            scratch_shapes=[dma((2 * LOOP + 3,))],
            compiler_params=pltpu.CompilerParams(vmem_limit_bytes=2**20),
            name="write_out",
        )(*done)
        return out.reshape(MATS, D, FF)

    spec = P(("rep", "dp"))
    return jax.shard_map(local, mesh=mesh, in_specs=(spec, spec), out_specs=P("rep"), check_vma=False)
```

```python
import jax
import jax.numpy as jnp
from jax import lax
from jax.experimental import pallas as pl
from jax.experimental.pallas import tpu as pltpu
from jax.sharding import PartitionSpec as P

T, D, FF, MATS = 8192, 640, 4096, 2
FC = 512
TK = 4096
KS = T // TK
PAIRS = MATS * FF // FC // 2
HALF = PAIRS // MATS
LOOP = PAIRS - 1
NG = 3
NA = 4
PR = D // 16
F32, BF16 = jnp.float32, jnp.bfloat16


class Plan:
    def __init__(self, groups, width, count, slots):
        self.groups, self.width, self.count, self.slots = groups, width, count, slots
        self.q = len(groups)
        self.n = [16]
        for g in groups:
            self.n.append(self.n[-1] >> len(g))
        self.lo, self.sem, at, sem = [], [], 0, 0
        for j, g in enumerate(groups):
            self.lo.append(at)
            self.sem.append(sem)
            at += ((1 << len(g)) - 1) * self.n[j + 1]
            sem += (1 << len(g)) - 1
        self.last, self.sems = at, sem
        self.stages = 2 * self.q + 2


PLANS = (
    Plan((("c",), ("x",), ("y", "w")), 512, LOOP, 2),
    Plan((("c",), ("y",), ("x", "w")), 512, LOOP, 2),
    Plan((("c",), ("x",), ("y", "w")), 512, 1, 1),
    Plan((("c",), ("y",), ("x", "w")), 256, 1, 1),
    Plan((("c",), ("x", "y", "w")), 256, 1, 1),
)
OFFSETS = ((0, 1, 3, 6, 9, 11, 13, 16), (0, 2, 4, 6, 10, 12, 14, 15))
DOT = None
ENDING = (
    (1, 0, 6), (1, 2, 5), (0, 3, 5), (1, 4, 4), (1, 5, 3), (0, 7, 3), DOT, (1, 1, 6), (0, 2, 6), (0, 5, 4), DOT,
    (2, 0, 0), (1, 3, 5), (0, 4, 5), (1, 5, 4), (2, 1, 0), (1, 6, 3), DOT, (3, 0, 0), (3, 1, 0), (1, 2, 6),
    (0, 3, 6), (1, 4, 5), (0, 6, 4), (1, 7, 3), DOT, (4, 0, 0), (2, 2, 0), (4, 1, 0), (1, 3, 6), (0, 4, 6),
    (0, 5, 5), (1, 6, 4), (0, 7, 4), (1, 7, 4), (3, 2, 0), (1, 5, 5), (2, 3, 0), (4, 2, 0), (1, 4, 6), (0, 6, 5),
    (0, 7, 5), (0, 5, 6), (3, 3, 0), (2, 4, 0), (4, 3, 0), (1, 6, 5), (1, 7, 5), (3, 4, 0), (1, 5, 6), (0, 6, 6),
    (2, 5, 0), (0, 7, 6), (4, 4, 0), (3, 5, 0), (4, 5, 0), (1, 6, 6), (2, 6, 0), (3, 6, 0), (1, 7, 6), (2, 7, 0),
    (3, 7, 0),
)
NP = len(PLANS)


def kernel(a_ref, g_ref, *rest):
    done, (ab, gb, acc), rest = rest[:NP], rest[NP:NP + 3], rest[NP + 3:]
    part, send, recv, rs_s, rs_r, ag_s, ag_r = (rest[i * NP:(i + 1) * NP] for i in range(7))
    asem, gsem = rest[7 * NP:]
    me = lax.axis_index("dp")
    bits = {"x": me // 16, "y": (me // 8) % 2, "h": (me // 4) % 2, "w": (me // 2) % 2, "c": me % 2}
    size = {"x": 16, "y": 8, "h": 4, "w": 2, "c": 1}

    def a_copy(n, k):
        rows = pl.ds(k * TK, TK)
        return pltpu.make_async_copy(a_ref.at[0, n, rows, :], ab.at[rows, :], asem.at[k])

    def g_copy(t):
        c, k = t // KS, t % KS
        rows = pl.ds(pl.multiple_of(k * TK, TK), TK)
        cols = pl.ds(pl.multiple_of((c % (2 * HALF)) * FC, FC), FC)
        return pltpu.make_async_copy(g_ref.at[0, c // (2 * HALF), rows, cols], gb.at[t % NG], gsem.at[t % NG])

    for k in range(KS):
        a_copy(0, k).start()
        g_copy(jnp.int32(k)).start()

    def flip(dims, m):
        value = 0
        for i, d in enumerate(dims):
            one = (m >> (len(dims) - 1 - i)) & 1
            value = value * 2 + (1 - bits[d] if one else bits[d])
        return value

    def peer(dims, m):
        to = me
        for i, d in enumerate(dims):
            if (m >> (len(dims) - 1 - i)) & 1:
                to = to + size[d] * (1 - 2 * bits[d])
        return (0, to)

    barrier = pltpu.get_barrier_semaphore()
    cube = ("x", "y", "w")
    partners = [peer(("c",), 1), peer(("h",), 1)] + [peer(cube, m) for m in range(1, 8)]
    for to in partners:
        pl.semaphore_signal(barrier, inc=1, device_id=to, device_id_type=pl.DeviceIdType.MESH)
    pl.semaphore_wait(barrier, len(partners))

    def remote(src, dst, ssem, rsem, to):
        return pltpu.make_async_remote_copy(
            src_ref=src, dst_ref=dst, send_sem=ssem, recv_sem=rsem,
            device_id=to, device_id_type=pl.DeviceIdType.MESH)

    def masks(plan, j):
        return range(1, 1 << len(plan.groups[j]))

    def rs_copy(pi, j, m, slot):
        plan = PLANS[pi]
        if j == plan.q:
            where, sem, to = pl.ds(plan.last, 1), plan.sems, peer(("h",), 1)
        else:
            n = plan.n[j + 1]
            where, sem, to = pl.ds(plan.lo[j] + (m - 1) * n, n), plan.sem[j] + m - 1, peer(plan.groups[j], m)
        return remote(send[pi].at[slot, where], recv[pi].at[slot, where],
                      rs_s[pi].at[sem, slot], rs_r[pi].at[sem, slot], to)

    def ag_copy(pi, j, m, c):
        plan = PLANS[pi]
        first = 0
        for i in range(j + 1):
            first = first + flip(plan.groups[i], 0) * plan.n[i + 1]
        where, sem = pl.ds(first, plan.n[j + 1]), plan.sem[j] + m - 1
        return remote(done[pi].at[c, where], done[pi].at[c, where],
                      ag_s[pi].at[sem, c], ag_r[pi].at[sem, c], peer(plan.groups[j], m))

    def stage(pi, s, c, tot):
        plan = PLANS[pi]
        q, w, slot = plan.q, plan.width, c % plan.slots

        def total(piece):
            return acc[tot, pl.ds(pl.multiple_of(piece * PR, 8), PR), :w]

        def value(p):
            v = total(flip(plan.groups[0], 0) * plan.n[1] + p) if s == 1 else part[pi][slot, p]
            for m in masks(plan, s - 1):
                v = v + recv[pi][slot, plan.lo[s - 1] + (m - 1) * plan.n[s] + p].astype(F32)
            return v

        if 1 <= s <= q:
            for m in masks(plan, s - 1):
                rs_copy(pi, s - 1, m, slot).wait()
        if s < q:
            n = plan.n[s + 1]
            for m in masks(plan, s):
                give = flip(plan.groups[s], m) * n
                for j in range(n):
                    v = total(give + j) if s == 0 else value(give + j)
                    send[pi][slot, plan.lo[s] + (m - 1) * n + j] = v.astype(BF16)
                rs_copy(pi, s, m, slot).start()
            if s > 0:
                keep = flip(plan.groups[s], 0) * n
                for j in range(n):
                    part[pi][slot, j] = value(keep + j)
        elif s == q:
            send[pi][slot, plan.last] = value(0).astype(BF16)
            rs_copy(pi, q, 0, slot).start()
        elif s == q + 1:
            rs_copy(pi, q, 0, slot).wait()
            mine = 0
            for i in range(q):
                mine = mine + flip(plan.groups[i], 0) * plan.n[i + 1]
            both = send[pi][slot, plan.last].astype(F32) + recv[pi][slot, plan.last].astype(F32)
            done[pi][c, mine] = both.astype(BF16)
        else:
            j = 2 * q + 1 - s
            for m in masks(plan, j):
                ag_copy(pi, j, m, c).wait()

    def gather(pi, s, c):
        plan = PLANS[pi]
        j = 2 * plan.q - s
        if 0 <= j < plan.q:
            for m in masks(plan, j):
                ag_copy(pi, j, m, c).start()

    def run(pi, s, c, tot):
        stage(pi, s, c, tot)
        if s > PLANS[pi].q:
            gather(pi, s, c)

    def dot(k, slot, cols):
        rows = slice(k * TK, (k + 1) * TK)
        return lax.dot_general(ab[rows, :], gb[slot, :, cols], (((0,), (0,)), ((), ())), preferred_element_type=F32)

    every = slice(0, FC)

    def pair(i, _):
        for u in range(2 * KS):
            which, k = u // KS, u % KS
            stages = [(OFFSETS[pi][s], pi, s) for pi in range(2) for s in range(PLANS[pi].stages)]
            for off, pi, s in sorted(stages, key=lambda v: (-v[0], v[1])):
                e = (pi + 1) * KS + off
                if e % (2 * KS) != u:
                    continue
                c = i - e // (2 * KS)

                @pl.when(c >= 0)
                def _():
                    run(pi, s, c, (2 * c + pi) % NA)

            t = i * 2 * KS + u
            g_copy(t + NG - 1).start()
            if which == 0:
                @pl.when(i % HALF == 0)
                def _():
                    a_copy(0, k).wait()

            g_copy(t).wait()
            tot = (2 * i + which) % NA
            if k == 0:
                acc[tot] = dot(k, t % NG, every)
            else:
                acc[tot] += dot(k, t % NG, every)
            if which == 1:
                @pl.when(i == HALF - 1)
                def _():
                    a_copy(1, k).start()
        return 0

    lax.fori_loop(0, LOOP, pair, 0)

    base = 2 * LOOP
    t0 = base * KS

    def tail_dot(step):
        if step < KS:
            if t0 + step + NG - 1 < 2 * PAIRS * KS:
                g_copy(jnp.int32(t0 + step + NG - 1)).start()
            g_copy(jnp.int32(t0 + step)).wait()
            d = dot(step, (t0 + step) % NG, every)
            if step == 0:
                acc[base % NA] = d
            else:
                acc[base % NA] += d
        else:
            part_of = step - KS
            cols = slice(part_of * 256, part_of * 256 + 256)
            for k in range(KS):
                if part_of == 0:
                    if t0 + KS + k + NG - 1 < 2 * PAIRS * KS:
                        g_copy(jnp.int32(t0 + KS + k + NG - 1)).start()
                    g_copy(jnp.int32(t0 + KS + k)).wait()
            tot = (base + 1 + part_of) % NA
            acc[tot, :, :256] = dot(0, (t0 + KS) % NG, cols) + dot(1, (t0 + KS + 1) % NG, cols)

    step = 0
    for item in ENDING:
        if item is DOT:
            tail_dot(step)
            step += 1
        else:
            pi, s, c = item
            run(pi, s, c, (2 * c + pi if pi < 2 else base + pi - 2) % NA)


def write_out(*refs):
    done, o_ref, sem = refs[:NP], refs[NP], refs[NP + 1]
    copies = []

    def copy(pi, c, at):
        w, per = PLANS[pi].width, FF
        cols = pl.ds(at % per, w)
        copies.append(pltpu.make_async_copy(
            done[pi].at[c], o_ref.at[at // per, :, :, cols], sem.at[len(copies)]))

    for c in range(LOOP):
        for pi in range(2):
            copy(pi, c, (2 * c + pi) * FC)
    at = 2 * LOOP * FC
    for pi in range(2, NP):
        copy(pi, 0, at)
        at += PLANS[pi].width
    for one in copies:
        one.start()
    for one in copies:
        one.wait()


def solution(mesh):
    dma = pltpu.SemaphoreType.DMA
    scratch = [pltpu.VMEM((T, D), BF16), pltpu.VMEM((NG, TK, FC), BF16), pltpu.VMEM((NA, D, FC), F32)]
    scratch += [pltpu.VMEM((p.slots, max(p.n[2], 1), PR, p.width), F32) for p in PLANS]
    scratch += [pltpu.VMEM((p.slots, 16, PR, p.width), BF16) for p in PLANS] * 2
    scratch += [dma((p.sems + 1, p.slots)) for p in PLANS] * 2
    scratch += [dma((p.sems, p.count)) for p in PLANS] * 2
    scratch += [dma((KS,)), dma((NG,))]
    shapes = [(p.count, 16, PR, p.width) for p in PLANS]

    def local(a, g):
        done = pl.pallas_call(
            kernel,
            out_shape=[pltpu.VMEM(s, BF16) for s in shapes],
            in_specs=[pl.BlockSpec(memory_space=pl.ANY)] * 2,
            out_specs=[pl.BlockSpec(memory_space=pltpu.VMEM)] * NP,
            scratch_shapes=scratch,
            compiler_params=pltpu.CompilerParams(
                collective_id=0, has_side_effects=True, vmem_limit_bytes=50 * 2**20),
            name="summed_grads",
        )(a, g)
        done = [pltpu.with_memory_space_constraint(d, pltpu.VMEM) for d in done]
        out = pl.pallas_call(
            write_out,
            out_shape=jax.ShapeDtypeStruct((MATS, 16, PR, FF), BF16),
            in_specs=[pl.BlockSpec(memory_space=pltpu.VMEM)] * NP,
            out_specs=pl.BlockSpec(memory_space=pl.ANY),
            scratch_shapes=[dma((2 * LOOP + 3,))],
            compiler_params=pltpu.CompilerParams(vmem_limit_bytes=2**20),
            name="write_out",
        )(*done)
        return out.reshape(MATS, D, FF)

    spec = P(("rep", "dp"))
    return jax.shard_map(local, mesh=mesh, in_specs=(spec, spec), out_specs=P("rep"), check_vma=False)
```
